32 devices in a mesh: view: 4 (over x, core), gz: 8 (over z, y).
Axes of the slice: x: 2, y: 2, z: 4, core: 2. Of those that a mesh axis runs over, the one named last changes fastest.
Arguments:
- views_data: float32 [4, 128, 128, 384], P('view', 'gz'), may hold values from 0.25 to 4
- start: float32 [128, 128, 384], P('gz'), may hold values from 0.5 to 2
- psf_table: float32 [8, 3, 17], replicated, may hold values from 0.05 to 1
- psf_index: int32 [4], P('view'), may hold values from 0 to 7
Outputs:
- estimate: float32 [128, 128, 384], P('gz')
The draws below stay inside these ranges and needn't reach their ends.
All inputs are finite; a program needn't handle non-finite values.
Results may differ from the reference program's by a relative error of at most 0.0001.
Values sent between devices are 32-bit elements; how exact they have to be, the bound alone decides.
No kernel may reach another device: no remote copies, remote signals or barrier semaphores. Data moves between devices by JAX's collectives and lax.ppermute only.
A program may use at most 128 MiB of HBM per device.

```python
import math
import jax
import jax.numpy as jnp
from jax import lax

NX = 128
NY = 384
RAD = 8
ITERS = 2
NPSF = 8
VIEWS = 4
TAPS = 17
NZ = 128


def plant(result, rng, least, high):
    extent = result.shape
    place = [jax.random.randint(jax.random.fold_in(rng, axis), (), 0, extent[axis]) for axis in range(len(extent))]
    result = result.at[tuple(place)].set(least)
    longest = extent.index(max(extent))
    place[longest] = (place[longest] + 1) % extent[longest]
    return result.at[tuple(place)].set(high)


def level_of(stream_key, shape, shards, smallest, high):
    def one(position, shards_of):
        steps = jax.random.uniform(jax.random.fold_in(jax.random.fold_in(stream_key, 6), position), (shards_of,), jnp.float32, smallest / len(shards), high / len(shards))
        return jnp.repeat(jnp.exp(steps), shape[position] // shards_of).reshape((-1,) + (1,) * (len(shape) - position - 1))

    gain = one(*shards[0])
    for cut in shards[1:]:
        gain = gain * one(*cut)
    return gain


def setup_inputs(seed: int = 0) -> dict:
    arg_keys = jax.random.split(jax.random.key(seed), 5)
    return {
        "views_data": jnp.clip(jnp.exp(math.log(4.0) - 2.7725887 * jax.random.uniform(arg_keys[0], (VIEWS, NZ, NX, NY), jnp.float32) ** level_of(arg_keys[0], (VIEWS, NZ, NX, NY), ((0, 4), (1, 8)), -0.2, 0.2)), 0.25, 4.0),
        "start": jnp.clip(jnp.exp(math.log(2.0) - 1.3862944 * jax.random.uniform(arg_keys[1], (NZ, NX, NY), jnp.float32) ** level_of(arg_keys[1], (NZ, NX, NY), ((0, 8),), -0.2, 0.2)), 0.5, 2.0),
        "psf_table": jnp.clip(jnp.exp(jax.random.uniform(arg_keys[2], (NPSF, 3, TAPS), jnp.float32, math.log(0.05), math.log(1.0))), 0.05, 1.0),
        "psf_index": plant(jax.random.randint(arg_keys[3], (VIEWS,), 0, NPSF), jax.random.fold_in(arg_keys[3], 1), 0, NPSF - 1).astype(jnp.int32),
    }


def band_matrix(kern_row, length):
    places = jnp.arange(length)
    offsets = places[None, :] - places[:, None]
    tap_shift = jnp.arange(2 * RAD + 1) - RAD
    matches = (offsets[None, :, :] == tap_shift[:, None, None]).astype(jnp.float32)
    return jnp.sum(kern_row[:, None, None] * matches, axis=0)


def blur_planes(volume, mat_x, mat_y):
    along_x = jnp.einsum("ij,zjy->ziy", mat_x, volume, precision=lax.Precision.HIGHEST)
    return jnp.einsum("zxj,ij->zxi", along_x, mat_y, precision=lax.Precision.HIGHEST)


def back_planes(volume, mat_x, mat_y):
    along_x = jnp.einsum("ij,ziy->zjy", mat_x, volume, precision=lax.Precision.HIGHEST)
    return jnp.einsum("zxi,ij->zxj", along_x, mat_y, precision=lax.Precision.HIGHEST)


def forward_z(padded, kern_z, rows):
    total = kern_z[0] * padded[0:rows]
    for tap in range(1, 2 * RAD + 1):
        total = total + kern_z[tap] * padded[tap:tap + rows]
    return total


def backward_z(padded, kern_z, rows):
    total = kern_z[0] * padded[2 * RAD:2 * RAD + rows]
    for tap in range(1, 2 * RAD + 1):
        total = total + kern_z[tap] * padded[2 * RAD - tap:2 * RAD - tap + rows]
    return total


def reference(views_data, start, psf_table, psf_index):
    estimate = start
    widths = ((RAD, RAD), (0, 0), (0, 0))
    for step in range(ITERS):
        total = None
        for which in range(VIEWS):
            kern = psf_table[psf_index[which]]
            kern = kern / jnp.sum(kern, axis=-1, keepdims=True)
            mat_x = band_matrix(kern[1], NX)
            mat_y = band_matrix(kern[2], NY)
            planes = blur_planes(estimate, mat_x, mat_y)
            blurred = forward_z(jnp.pad(planes, widths), kern[0], NZ)
            ratio = views_data[which] / blurred
            smeared = backward_z(jnp.pad(ratio, widths), kern[0], NZ)
            correction = back_planes(smeared, mat_x, mat_y)
            total = correction if total is None else total * correction
        estimate = estimate * jnp.power(total, 1.0 / VIEWS)
    return estimate
```

```python
import functools

import jax
import jax.numpy as jnp
from jax import lax
from jax.experimental import pallas as pl
from jax.experimental.pallas import tpu as pltpu
from jax.sharding import PartitionSpec as P

ITERS = 2
LANES = 128
SUBLANES = 8
AXES = ("view", "gz")


def split_bf16(value):
    high = value.astype(jnp.bfloat16)
    low = (value - high.astype(jnp.float32)).astype(jnp.bfloat16)
    return high, low


def dot3(left, right_high, right_low):
    high, low = split_bf16(left)
    dot = functools.partial(jnp.dot, preferred_element_type=jnp.float32)
    return dot(high, right_high) + (dot(low, right_high) + dot(high, right_low))


def blur_z(pieces, taps_ref, flipped, store, planes, rows, cols):
    taps = taps_ref.shape[0]
    coeffs = [taps_ref[taps - 1 - t if flipped else t] for t in range(taps)]
    where = [(ref, z) for ref in pieces for z in range(ref.shape[0])]

    def chunk(r, carry):
        row = pl.ds(pl.multiple_of(r * SUBLANES, SUBLANES), SUBLANES)
        for c in range(cols // LANES):
            col = slice(c * LANES, (c + 1) * LANES)
            held = [ref[z, row, col] for ref, z in where]
            for out in range(planes):
                total = coeffs[0] * held[out]
                for t in range(1, taps):
                    total = total + coeffs[t] * held[out + t]
                store(out, row, col, total)
        return carry

    lax.fori_loop(0, rows // SUBLANES, chunk, 0)


def ratio_kernel(taps_ref, wide_ref, band_x_ref, fwd_y_ref, back_y_ref, data_ref, out_ref, z_ref, x_ref):
    planes, rows, cols = out_ref.shape

    def store(out, row, col, value):
        z_ref[out, row, col] = value

    blur_z([wide_ref], taps_ref, False, store, planes, z_ref.shape[1], cols)
    band_x = band_x_ref[...]
    for z in range(planes):
        high, low = split_bf16(z_ref[z])
        stacked = jnp.concatenate([high, low, high], axis=0)
        x_ref[z] = jnp.dot(band_x, stacked, preferred_element_type=jnp.float32)
    fwd_high, fwd_low = split_bf16(fwd_y_ref[...])
    back_high, back_low = split_bf16(back_y_ref[...])
    step = planes // 2
    for at in range(0, planes, step):
        part = x_ref[at : at + step].reshape(step * rows, cols)
        blurred = dot3(part, fwd_high, fwd_low)
        ratio = data_ref[at : at + step].reshape(step * rows, cols) / blurred
        out_ref[at : at + step] = dot3(ratio, back_high, back_low).reshape(step, rows, cols)


def back_z_kernel(taps_ref, low_ref, mid_ref, high_ref, out_ref):
    planes, rows, cols = out_ref.shape

    def store(out, row, col, value):
        out_ref[out, row, col] = value

    blur_z([low_ref, mid_ref, high_ref], taps_ref, True, store, planes, rows, cols)


def back_x_kernel(odd_ref, band_x_ref, flip_low_ref, step_low_ref, mid_ref, flip_high_ref, step_high_ref, prod_ref, out_ref):
    band_x = band_x_ref[...]
    odd = odd_ref[0] == 1
    for z in range(out_ref.shape[0]):
        low = jnp.where(odd, flip_low_ref[z], step_low_ref[z])
        high = jnp.where(odd, step_high_ref[z], flip_high_ref[z])
        wide = jnp.concatenate([low, mid_ref[z], high], axis=0)
        high, low = split_bf16(wide)
        stacked = jnp.concatenate([high, low, high], axis=0)
        part = jnp.dot(band_x, stacked, preferred_element_type=jnp.float32)
        out_ref[z] = part if prod_ref is None else prod_ref[z] * part


def first_back_x_kernel(*refs):
    back_x_kernel(*refs[:-1], None, refs[-1])


def call(kernel, shape, operands, scratch=(), smem=0):
    specs = [pl.BlockSpec(memory_space=pltpu.SMEM)] * smem
    specs += [pl.BlockSpec(memory_space=pltpu.VMEM)] * (len(operands) - smem)
    return pl.pallas_call(
        kernel,
        out_shape=jax.ShapeDtypeStruct(shape, jnp.float32),
        in_specs=specs,
        out_specs=pl.BlockSpec(memory_space=pltpu.VMEM),
        scratch_shapes=[pltpu.VMEM(s, jnp.float32) for s in scratch],
    )(*operands)


def bands(kern_rows, height, width, shift):
    offsets = jnp.arange(width)[None, :] - jnp.arange(height)[:, None] + shift
    total = jnp.zeros((kern_rows.shape[0], height, width), jnp.float32)
    for tap in range(kern_rows.shape[1]):
        total = jnp.where(offsets[None] == tap, kern_rows[:, tap, None, None], total)
    return total


def stacked_bands(matrix):
    high = lax.reduce_precision(matrix, 8, 7)
    return jnp.concatenate([high, high, matrix - high], axis=2).astype(jnp.bfloat16)


def make_on_device(mesh):
    views, slabs = mesh.shape["view"], mesh.shape["gz"]
    outer = views // 2
    parts = views
    devices = [(a, c, k, b) for a in range(outer) for c in range(2) for k in range(slabs // 2) for b in range(2)]

    def index(a, c, k, b):
        return (a * 2 + c) * slabs + k * 2 + b

    def part_of(a, b):
        return a * 2 + ((a ^ b) & 1)

    def move(value, pairs):
        return lax.ppermute(value, AXES, [(index(*s), index(*d)) for s, d in pairs])

    owner = {}
    for a, c, k, b in devices:
        owner[(part_of(a, b), k * 2 + c)] = (a, c, k, b)

    def shifted(rows_by, planes_by):
        pairs = []
        for (part, slab), device in owner.items():
            target = owner.get((part + rows_by, slab + planes_by))
            if target is not None:
                pairs.append((device, target))
        return pairs

    x_up, x_down = shifted(1, 0), shifted(-1, 0)
    z_up, z_down = shifted(0, 1), shifted(0, -1)

    def on_device(views_data, start, psf_table, psf_index):
        slab = views_data[0]
        planes, width_x, width_y = start.shape
        taps = psf_table.shape[2]
        radius = (taps - 1) // 2
        rows = width_x // parts
        v, g = lax.axis_index("view"), lax.axis_index("gz")
        a, c, b = v // 2, v % 2, g % 2

        def rows_at(value, part):
            return lax.dynamic_slice_in_dim(value, part * rows, rows, 1)

        away = [((A, C, K, B), (A, C, K, 1 - B)) for A, C, K, B in devices if B == C]
        other = move(rows_at(start, part_of(a, 1 - b)), away)
        estimate = jnp.where(b == c, rows_at(start, part_of(a, b)), other)

        slots = [(s, t) for s in range(outer) for t in range(2)]
        held = []
        for s, t in slots:
            pairs = [((A, C, K, B), ((A + s) % outer, B, K, C ^ t)) for A, C, K, B in devices]
            held.append(move(rows_at(slab, part_of((a + s) % outer, c ^ t)), pairs))
        which = jnp.stack([((a - s) % outer) * 2 + (b ^ t) for s, t in slots])
        indices = lax.all_gather(psf_index, "view", tiled=True)
        mine = jnp.sum(jnp.where(which[:, None] == jnp.arange(views)[None, :], indices[None, :], 0), axis=1)
        picked = (jnp.arange(psf_table.shape[0])[None, :] == mine[:, None]).astype(jnp.float32)
        kern = jnp.sum(picked[:, :, None, None] * psf_table[None], axis=1)
        kern = kern / jnp.sum(kern, axis=-1, keepdims=True)
        turned = kern[:, :, ::-1]
        wide_rows = rows + 2 * radius
        fwd_x = stacked_bands(bands(kern[:, 1], rows, wide_rows, 0))
        back_x = stacked_bands(bands(turned[:, 1], rows, wide_rows, 0))
        back_y = bands(kern[:, 2], width_y, width_y, radius)
        fwd_y = bands(turned[:, 2], width_y, width_y, radius)

        block = (planes, rows, width_y)
        odd = (part_of(a, b) % 2).astype(jnp.int32).reshape(1)
        for step in range(ITERS):
            low = move(estimate[:, rows - radius :], x_up)
            high = move(estimate[:, :radius], x_down)
            wide = jnp.concatenate([low, estimate, high], axis=1)
            low = move(wide[planes - radius :], z_up)
            high = move(wide[:radius], z_down)
            wide = jnp.concatenate([low, wide, high], axis=0)
            smeared, lows, highs = {}, {}, {}
            for n, slot in enumerate(slots):
                ratio = call(
                    ratio_kernel,
                    block,
                    (kern[n, 0], wide, fwd_x[n], fwd_y[n], back_y[n], held[n]),
                    scratch=((planes, wide_rows, width_y), block),
                    smem=1,
                )
                low = move(ratio[planes - radius :], z_up)
                high = move(ratio[:radius], z_down)
                smeared[slot] = call(back_z_kernel, block, (kern[n, 0], low, ratio, high), smem=1)
                lows[slot] = move(smeared[slot][:, rows - radius :], x_up)
                highs[slot] = move(smeared[slot][:, :radius], x_down)
            total = None
            for n, (s, t) in enumerate(slots):
                operands = (
                    odd,
                    back_x[n],
                    lows[s, t ^ 1],
                    lows[(s - 1) % outer, t],
                    smeared[s, t],
                    highs[s, t ^ 1],
                    highs[(s + 1) % outer, t],
                )
                if total is None:
                    total = call(first_back_x_kernel, block, operands, smem=1)
                else:
                    total = call(back_x_kernel, block, operands + (total,), smem=1)
            estimate = estimate * jnp.power(total, 1.0 / views)

        half = planes // 2
        result = jnp.zeros((planes, width_x, width_y), jnp.float32)
        across = [((A, C, K, B), (A, 1 - C, K, B)) for A, C, K, B in devices]
        for s, t in slots:
            pairs = [((A, C, K, B), ((A + s) % outer, B ^ t, K, C)) for A, C, K, B in devices]
            piece = move(lax.dynamic_slice_in_dim(estimate, (b ^ t) * half, half, 0), pairs)
            twin = move(piece, across)
            from_a = (a - s) % outer
            result = lax.dynamic_update_slice(result, piece, (c * half, part_of(from_a, c ^ t) * rows, 0))
            result = lax.dynamic_update_slice(
                result, twin, ((1 - c) * half, part_of(from_a, (1 - c) ^ t) * rows, 0)
            )
        return result

    return on_device


def solution(mesh):
    return jax.shard_map(
        make_on_device(mesh),
        mesh=mesh,
        in_specs=(P("view", "gz", None, None), P("gz", None, None), P(), P("view")),
        out_specs=P("gz", None, None),
        check_vma=False,
    )
```

```python
import functools

import jax
import jax.numpy as jnp
from jax import lax
from jax.experimental import pallas as pl
from jax.experimental.pallas import tpu as pltpu
from jax.sharding import PartitionSpec as P

ITERS = 2
LANES = 128
SUBLANES = 8
AXES = ("view", "gz")


def split_bf16(value):
    high = value.astype(jnp.bfloat16)
    low = (value - high.astype(jnp.float32)).astype(jnp.bfloat16)
    return high, low


def dot3(left, right_high, right_low):
    high, low = split_bf16(left)
    dot = functools.partial(jnp.dot, preferred_element_type=jnp.float32)
    return dot(high, right_high) + (dot(low, right_high) + dot(high, right_low))


def blur_z(pieces, lead, taps_ref, flipped, store, planes, rows, cols):
    taps = taps_ref.shape[1]
    coeffs = [taps_ref[lead, taps - 1 - t if flipped else t] for t in range(taps)]
    where = [(ref, z) for ref in pieces for z in range(ref.shape[-3])]
    columns = cols // LANES

    def chunk(at, carry):
        row = pl.ds(pl.multiple_of((at // columns) * SUBLANES, SUBLANES), SUBLANES)
        col = pl.ds(pl.multiple_of((at % columns) * LANES, LANES), LANES)
        held = [ref[z, row, col] if len(ref.shape) == 3 else ref[lead, z, row, col] for ref, z in where]
        for out in range(planes):
            total = coeffs[0] * held[out]
            for t in range(1, taps):
                total = total + coeffs[t] * held[out + t]
            store(out, row, col, total)
        return carry

    lax.fori_loop(0, rows // SUBLANES * columns, chunk, 0)


def ratio_kernel(taps_ref, wide_ref, band_x_ref, fwd_y_ref, back_y_ref, *refs):
    group = band_x_ref.shape[0]
    data_refs, (out_ref, up_ref, down_ref, z_ref, x_ref) = refs[:group], refs[group:]
    planes, rows, cols = out_ref.shape[1:]
    radius = up_ref.shape[1]

    def store(out, row, col, value):
        z_ref[out, row, col] = value

    for n in range(group):
        blur_z([wide_ref], n, taps_ref, False, store, planes, z_ref.shape[1], cols)
        band_x = band_x_ref[n]
        for z in range(planes):
            high, low = split_bf16(z_ref[z])
            stacked = jnp.concatenate([high, low, high], axis=0)
            x_ref[z] = jnp.dot(band_x, stacked, preferred_element_type=jnp.float32)
        fwd_high, fwd_low = split_bf16(fwd_y_ref[n])
        back_high, back_low = split_bf16(back_y_ref[n])
        step = planes // 2
        for at in range(0, planes, step):
            part = x_ref[at : at + step].reshape(step * rows, cols)
            blurred = dot3(part, fwd_high, fwd_low)
            ratio = data_refs[n][at : at + step].reshape(step * rows, cols) / blurred
            out_ref[n, at : at + step] = dot3(ratio, back_high, back_low).reshape(step, rows, cols)
        up_ref[n] = out_ref[n, planes - radius :]
        down_ref[n] = out_ref[n, :radius]


def back_z_kernel(taps_ref, low_ref, mid_ref, high_ref, out_ref, up_ref, down_ref):
    group, planes, rows, cols = out_ref.shape
    radius = up_ref.shape[2]

    def one(n, carry):
        def store(out, row, col, value):
            out_ref[n, out, row, col] = value

        blur_z([low_ref, mid_ref, high_ref], n, taps_ref, True, store, planes, rows, cols)
        up_ref[n] = out_ref[n, :, rows - radius :]
        down_ref[n] = out_ref[n, :, :radius]
        return carry

    lax.fori_loop(0, group, one, 0)


def update_kernel(odd_ref, band_x_ref, estimate_ref, *refs):
    (out_ref, up_ref, down_ref), refs = refs[-3:], refs[:-3]
    outer = len(refs) // 3
    mids, lows, highs = refs[:outer], refs[outer : 2 * outer], refs[2 * outer :]
    planes, rows, cols = out_ref.shape
    radius = up_ref.shape[1]
    odd = odd_ref[0] == 1
    group = mids[0].shape[0]
    bands_x = [band_x_ref[n] for n in range(outer * group)]

    def plane(z, carry):
        total = None
        for s in range(outer):
            for t in range(group):
                below = jnp.where(odd, lows[s][t ^ 1, z], lows[(s - 1) % outer][t, z])
                above = jnp.where(odd, highs[(s + 1) % outer][t, z], highs[s][t ^ 1, z])
                wide = jnp.concatenate([below, mids[s][t, z], above], axis=0)
                high, low = split_bf16(wide)
                stacked = jnp.concatenate([high, low, high], axis=0)
                part = jnp.dot(bands_x[s * group + t], stacked, preferred_element_type=jnp.float32)
                total = part if total is None else total * part
        updated = estimate_ref[z] * jnp.exp(jnp.log(total) * (1.0 / (outer * group)))
        out_ref[z] = updated
        up_ref[z] = updated[rows - radius :]
        down_ref[z] = updated[:radius]
        return carry

    lax.fori_loop(0, planes, plane, 0, unroll=2)


def call(kernel, shapes, operands, scratch=()):
    specs = [pl.BlockSpec(memory_space=pltpu.SMEM)]
    specs += [pl.BlockSpec(memory_space=pltpu.VMEM)] * (len(operands) - 1)
    return pl.pallas_call(
        kernel,
        out_shape=[jax.ShapeDtypeStruct(s, jnp.float32) for s in shapes],
        in_specs=specs,
        out_specs=[pl.BlockSpec(memory_space=pltpu.VMEM)] * len(shapes),
        scratch_shapes=[pltpu.VMEM(s, jnp.float32) for s in scratch],
    )(*operands)


def bands(kern_rows, height, width, shift):
    offsets = jnp.arange(width)[None, :] - jnp.arange(height)[:, None] + shift
    total = jnp.zeros((kern_rows.shape[0], height, width), jnp.float32)
    for tap in range(kern_rows.shape[1]):
        total = jnp.where(offsets[None] == tap, kern_rows[:, tap, None, None], total)
    return total


def stacked_bands(matrix):
    high = lax.reduce_precision(matrix, 8, 7)
    return jnp.concatenate([high, high, matrix - high], axis=2).astype(jnp.bfloat16)


def make_on_device(mesh):
    views, slabs = mesh.shape["view"], mesh.shape["gz"]
    outer = views // 2
    parts = views
    devices = [(a, c, k, b) for a in range(outer) for c in range(2) for k in range(slabs // 2) for b in range(2)]

    def index(a, c, k, b):
        return (a * 2 + c) * slabs + k * 2 + b

    def part_of(a, b):
        return a * 2 + ((a ^ b) & 1)

    def move(value, pairs):
        return lax.ppermute(value, AXES, [(index(*s), index(*d)) for s, d in pairs])

    owner = {}
    for a, c, k, b in devices:
        owner[(part_of(a, b), k * 2 + c)] = (a, c, k, b)

    def shifted(rows_by, planes_by):
        pairs = []
        for (part, slab), device in owner.items():
            target = owner.get((part + rows_by, slab + planes_by))
            if target is not None:
                pairs.append((device, target))
        return pairs

    x_up, x_down = shifted(1, 0), shifted(-1, 0)
    z_up, z_down = shifted(0, 1), shifted(0, -1)

    def on_device(views_data, start, psf_table, psf_index):
        slab = views_data[0]
        planes, width_x, width_y = start.shape
        taps = psf_table.shape[2]
        radius = (taps - 1) // 2
        rows = width_x // parts
        v, g = lax.axis_index("view"), lax.axis_index("gz")
        a, c, b = v // 2, v % 2, g % 2

        def rows_at(value, part):
            return lax.dynamic_slice_in_dim(value, part * rows, rows, 1)

        indices = lax.all_gather(psf_index, "view", tiled=True)
        slab, start, indices = lax.optimization_barrier((slab, start, indices))

        def rows_around(value, part):
            at = part * rows
            low = lax.dynamic_slice_in_dim(value, jnp.maximum(at - radius, 0), radius, 1)
            mid = lax.dynamic_slice_in_dim(value, at, rows, 1)
            high = lax.dynamic_slice_in_dim(value, jnp.minimum(at + rows, width_x - radius), radius, 1)
            low = jnp.where(part > 0, low, 0.0)
            high = jnp.where(part < parts - 1, high, 0.0)
            return jnp.concatenate([low, mid, high], axis=1)

        def from_slab(value, offset):
            pairs = []
            for A, C, K, B in devices:
                slab_to = 2 * K + B + offset
                if 0 <= slab_to < slabs:
                    pairs.append(((A, C, K, B), (A, slab_to % 2, slab_to // 2, C)))
            return move(value, pairs)

        whole = rows_around(start, part_of(a, c))
        own = from_slab(whole, 0)
        low = from_slab(whole[planes - radius :], 1)
        high = from_slab(whole[:radius], -1)
        wide = jnp.concatenate([low, own, high], axis=0)
        estimate = own[:, radius : radius + rows]

        slots = [(s, t) for s in range(outer) for t in range(2)]
        held = []
        for s, t in slots:
            pairs = [((A, C, K, B), ((A + s) % outer, B, K, C ^ t)) for A, C, K, B in devices]
            held.append(move(rows_at(slab, part_of((a + s) % outer, c ^ t)), pairs))
        which = jnp.stack([((a - s) % outer) * 2 + (b ^ t) for s, t in slots])
        mine = jnp.sum(jnp.where(which[:, None] == jnp.arange(views)[None, :], indices[None, :], 0), axis=1)
        picked = (jnp.arange(psf_table.shape[0])[None, :] == mine[:, None]).astype(jnp.float32)
        kern = jnp.sum(picked[:, :, None, None] * psf_table[None], axis=1)
        kern = kern / jnp.sum(kern, axis=-1, keepdims=True)
        turned = kern[:, :, ::-1]
        wide_rows = rows + 2 * radius
        fwd_x = stacked_bands(bands(kern[:, 1], rows, wide_rows, 0))
        back_x = stacked_bands(bands(turned[:, 1], rows, wide_rows, 0))
        back_y = bands(kern[:, 2], width_y, width_y, radius)
        fwd_y = bands(turned[:, 2], width_y, width_y, radius)

        block = (planes, rows, width_y)
        odd = (part_of(a, b) % 2).astype(jnp.int32).reshape(1)
        edge_z, edge_x = (2, radius, rows, width_y), (2, planes, radius, width_y)
        for step in range(ITERS):
            if step:
                low, high = move(up, x_up), move(down, x_down)
                wide = jnp.concatenate([low, estimate, high], axis=1)
                low = move(wide[planes - radius :], z_up)
                high = move(wide[:radius], z_down)
                wide = jnp.concatenate([low, wide, high], axis=0)
            ratios = []
            for s in range(outer):
                n = slice(2 * s, 2 * s + 2)
                ratio, up, down = call(
                    ratio_kernel,
                    ((2,) + block, edge_z, edge_z),
                    (kern[n, 0], wide, fwd_x[n], fwd_y[n], back_y[n], *held[n]),
                    scratch=((planes, wide_rows, width_y), block),
                )
                ratios.append((move(up, z_up), ratio, move(down, z_down)))
            mids, lows, highs = [], [], []
            for s in range(outer):
                smeared, up, down = call(
                    back_z_kernel, ((2,) + block, edge_x, edge_x), (kern[2 * s : 2 * s + 2, 0], *ratios[s])
                )
                mids.append(smeared)
                lows.append(move(up, x_up))
                highs.append(move(down, x_down))
            estimate, up, down = call(
                update_kernel,
                (block, (planes, radius, width_y), (planes, radius, width_y)),
                (odd, back_x, estimate, *mids, *lows, *highs),
            )

        half = planes // 2
        result = jnp.zeros((planes, width_x, width_y), jnp.float32)
        across = [((A, C, K, B), (A, 1 - C, K, B)) for A, C, K, B in devices]
        for s, t in slots:
            pairs = [((A, C, K, B), ((A + s) % outer, B ^ t, K, C)) for A, C, K, B in devices]
            piece = move(lax.dynamic_slice_in_dim(estimate, (b ^ t) * half, half, 0), pairs)
            twin = move(piece, across)
            from_a = (a - s) % outer
            result = lax.dynamic_update_slice(result, piece, (c * half, part_of(from_a, c ^ t) * rows, 0))
            result = lax.dynamic_update_slice(
                result, twin, ((1 - c) * half, part_of(from_a, (1 - c) ^ t) * rows, 0)
            )
        return result

    return on_device


def solution(mesh):
    return jax.shard_map(
        make_on_device(mesh),
        mesh=mesh,
        in_specs=(P("view", "gz", None, None), P("gz", None, None), P(), P("view")),
        out_specs=P("gz", None, None),
        check_vma=False,
    )
```

```python
import functools

import jax
import jax.numpy as jnp
from jax import lax
from jax.experimental import pallas as pl
from jax.experimental.pallas import tpu as pltpu
from jax.sharding import PartitionSpec as P

ITERS = 2
LANES = 128
SUBLANES = 8
AXES = ("view", "gz")


def split_bf16(value):
    high = value.astype(jnp.bfloat16)
    low = (value - high.astype(jnp.float32)).astype(jnp.bfloat16)
    return high, low


def dot3(left, right_high, right_low):
    high, low = split_bf16(left)
    dot = functools.partial(jnp.dot, preferred_element_type=jnp.float32)
    return dot(high, right_high) + (dot(low, right_high) + dot(high, right_low))


def blur_z(pieces, lead, taps_ref, flipped, store, planes, rows, cols):
    taps = taps_ref.shape[1]
    coeffs = [taps_ref[lead, taps - 1 - t if flipped else t] for t in range(taps)]
    where = [(ref, z) for ref in pieces for z in range(ref.shape[-3])]
    columns = cols // LANES

    def chunk(at, carry):
        row = pl.ds(pl.multiple_of((at // columns) * SUBLANES, SUBLANES), SUBLANES)
        col = pl.ds(pl.multiple_of((at % columns) * LANES, LANES), LANES)
        held = [ref[z, row, col] if len(ref.shape) == 3 else ref[lead, z, row, col] for ref, z in where]
        for out in range(planes):
            total = coeffs[0] * held[out]
            for t in range(1, taps):
                total = total + coeffs[t] * held[out + t]
            store(out, row, col, total)
        return carry

    lax.fori_loop(0, rows // SUBLANES * columns, chunk, 0)


def ratio_kernel(taps_ref, wide_ref, band_x_ref, fwd_y_ref, back_y_ref, *refs):
    group = band_x_ref.shape[0]
    data_refs, (out_ref, up_ref, down_ref, z_ref, x_ref) = refs[:group], refs[group:]
    planes, rows, cols = out_ref.shape[1:]
    radius = up_ref.shape[1]

    def store(out, row, col, value):
        z_ref[out, row, col] = value

    for n in range(group):
        blur_z([wide_ref], n, taps_ref, False, store, planes, z_ref.shape[1], cols)
        band_x = band_x_ref[n]
        for z in range(planes):
            high, low = split_bf16(z_ref[z])
            stacked = jnp.concatenate([high, low, high], axis=0)
            x_ref[z] = jnp.dot(band_x, stacked, preferred_element_type=jnp.float32)
        fwd_high, fwd_low = split_bf16(fwd_y_ref[n])
        back_high, back_low = split_bf16(back_y_ref[n])
        step = planes // 2
        for at in range(0, planes, step):
            part = x_ref[at : at + step].reshape(step * rows, cols)
            blurred = dot3(part, fwd_high, fwd_low)
            ratio = data_refs[n][at : at + step].reshape(step * rows, cols) / blurred
            out_ref[n, at : at + step] = dot3(ratio, back_high, back_low).reshape(step, rows, cols)
        up_ref[n] = out_ref[n, planes - radius :]
        down_ref[n] = out_ref[n, :radius]


def back_z_kernel(taps_ref, low_ref, mid_ref, high_ref, out_ref, up_ref, down_ref):
    group, planes, rows, cols = out_ref.shape
    radius = up_ref.shape[2]

    def one(n, carry):
        def store(out, row, col, value):
            out_ref[n, out, row, col] = value

        blur_z([low_ref, mid_ref, high_ref], n, taps_ref, True, store, planes, rows, cols)
        up_ref[n] = out_ref[n, :, rows - radius :]
        down_ref[n] = out_ref[n, :, :radius]
        return carry

    lax.fori_loop(0, group, one, 0)


def update_kernel(odd_ref, band_x_ref, estimate_ref, *refs):
    (out_ref, up_ref, down_ref), refs = refs[-3:], refs[:-3]
    outer = len(refs) // 3
    mids, lows, highs = refs[:outer], refs[outer : 2 * outer], refs[2 * outer :]
    planes, rows, cols = out_ref.shape
    radius = up_ref.shape[1]
    odd = odd_ref[0] == 1
    group = mids[0].shape[0]
    bands_x = [band_x_ref[n] for n in range(outer * group)]

    def plane(z, carry):
        total = None
        for s in range(outer):
            for t in range(group):
                below = jnp.where(odd, lows[s][t ^ 1, z], lows[(s - 1) % outer][t, z])
                above = jnp.where(odd, highs[(s + 1) % outer][t, z], highs[s][t ^ 1, z])
                wide = jnp.concatenate([below, mids[s][t, z], above], axis=0)
                high, low = split_bf16(wide)
                stacked = jnp.concatenate([high, low, high], axis=0)
                part = jnp.dot(bands_x[s * group + t], stacked, preferred_element_type=jnp.float32)
                total = part if total is None else total * part
        updated = estimate_ref[z] * jnp.exp(jnp.log(total) * (1.0 / (outer * group)))
        out_ref[z] = updated
        up_ref[z] = updated[rows - radius :]
        down_ref[z] = updated[:radius]
        return carry

    lax.fori_loop(0, planes, plane, 0, unroll=2)


def call(kernel, shapes, operands, scratch=()):
    specs = [pl.BlockSpec(memory_space=pltpu.SMEM)]
    specs += [pl.BlockSpec(memory_space=pltpu.VMEM)] * (len(operands) - 1)
    return pl.pallas_call(
        kernel,
        out_shape=[jax.ShapeDtypeStruct(s, jnp.float32) for s in shapes],
        in_specs=specs,
        out_specs=[pl.BlockSpec(memory_space=pltpu.VMEM)] * len(shapes),
        scratch_shapes=[pltpu.VMEM(s, jnp.float32) for s in scratch],
    )(*operands)


def bands(kern_rows, height, width, shift):
    offsets = jnp.arange(width)[None, :] - jnp.arange(height)[:, None] + shift
    total = jnp.zeros((kern_rows.shape[0], height, width), jnp.float32)
    for tap in range(kern_rows.shape[1]):
        total = jnp.where(offsets[None] == tap, kern_rows[:, tap, None, None], total)
    return total


def stacked_bands(matrix):
    high = lax.reduce_precision(matrix, 8, 7)
    return jnp.concatenate([high, high, matrix - high], axis=2).astype(jnp.bfloat16)


def make_on_device(mesh):
    views, slabs = mesh.shape["view"], mesh.shape["gz"]
    outer = views // 2
    parts = views
    devices = [(a, c, k, b) for a in range(outer) for c in range(2) for k in range(slabs // 2) for b in range(2)]

    def index(a, c, k, b):
        return (a * 2 + c) * slabs + k * 2 + b

    def part_of(a, b):
        return a * 2 + ((a ^ b) & 1)

    def move(value, pairs):
        return lax.ppermute(value, AXES, [(index(*s), index(*d)) for s, d in pairs])

    owner = {}
    for a, c, k, b in devices:
        owner[(part_of(a, b), k * 2 + c)] = (a, c, k, b)

    def shifted(rows_by, planes_by):
        pairs = []
        for (part, slab), device in owner.items():
            target = owner.get((part + rows_by, slab + planes_by))
            if target is not None:
                pairs.append((device, target))
        return pairs

    x_up, x_down = shifted(1, 0), shifted(-1, 0)
    z_up, z_down = shifted(0, 1), shifted(0, -1)

    def on_device(views_data, start, psf_table, psf_index):
        slab = views_data[0]
        planes, width_x, width_y = start.shape
        taps = psf_table.shape[2]
        radius = (taps - 1) // 2
        rows = width_x // parts
        v, g = lax.axis_index("view"), lax.axis_index("gz")
        a, c, b = v // 2, v % 2, g % 2

        def rows_at(value, part):
            return lax.dynamic_slice_in_dim(value, part * rows, rows, 1)

        indices = lax.all_gather(psf_index, "view", tiled=True)
        slab, start, indices = lax.optimization_barrier((slab, start, indices))

        def rows_around(value, part):
            at = part * rows
            low = lax.dynamic_slice_in_dim(value, jnp.maximum(at - radius, 0), radius, 1)
            mid = lax.dynamic_slice_in_dim(value, at, rows, 1)
            high = lax.dynamic_slice_in_dim(value, jnp.minimum(at + rows, width_x - radius), radius, 1)
            low = jnp.where(part > 0, low, 0.0)
            high = jnp.where(part < parts - 1, high, 0.0)
            return jnp.concatenate([low, mid, high], axis=1)

        def from_slab(value, offset):
            pairs = []
            for A, C, K, B in devices:
                slab_to = 2 * K + B + offset
                if 0 <= slab_to < slabs:
                    pairs.append(((A, C, K, B), (A, slab_to % 2, slab_to // 2, C)))
            return move(value, pairs)

        whole = rows_around(start, part_of(a, c))
        own = from_slab(whole, 0)
        low = from_slab(whole[planes - radius :], 1)
        high = from_slab(whole[:radius], -1)
        slots = [(s, t) for s in range(outer) for t in range(2)]
        held = []
        for s, t in slots:
            if (s, t) == (1, 0):
                slab, low = lax.optimization_barrier((slab, low))
            pairs = [((A, C, K, B), ((A + s) % outer, B, K, C ^ t)) for A, C, K, B in devices]
            held.append(move(rows_at(slab, part_of((a + s) % outer, c ^ t)), pairs))
        which = jnp.stack([((a - s) % outer) * 2 + (b ^ t) for s, t in slots])
        mine = jnp.sum(jnp.where(which[:, None] == jnp.arange(views)[None, :], indices[None, :], 0), axis=1)
        picked = (jnp.arange(psf_table.shape[0])[None, :] == mine[:, None]).astype(jnp.float32)
        kern = jnp.sum(picked[:, :, None, None] * psf_table[None], axis=1)
        kern = kern / jnp.sum(kern, axis=-1, keepdims=True)
        turned = kern[:, :, ::-1]
        wide_rows = rows + 2 * radius
        fwd_x = stacked_bands(bands(kern[:, 1], rows, wide_rows, 0))
        back_x = stacked_bands(bands(turned[:, 1], rows, wide_rows, 0))
        back_y = bands(kern[:, 2], width_y, width_y, radius)
        fwd_y = bands(turned[:, 2], width_y, width_y, radius)

        wide = jnp.concatenate([low, own, high], axis=0)
        estimate = own[:, radius : radius + rows]
        block = (planes, rows, width_y)
        odd = (part_of(a, b) % 2).astype(jnp.int32).reshape(1)
        edge_z, edge_x = (2, radius, rows, width_y), (2, planes, radius, width_y)
        for step in range(ITERS):
            if step:
                low, high = move(up, x_up), move(down, x_down)
                wide = jnp.concatenate([low, estimate, high], axis=1)
                low = move(wide[planes - radius :], z_up)
                high = move(wide[:radius], z_down)
                wide = jnp.concatenate([low, wide, high], axis=0)
            ratios = []
            for s in range(outer):
                n = slice(2 * s, 2 * s + 2)
                taps_z = kern[n, 0]
                if ratios:
                    taps_z, _ = lax.optimization_barrier((taps_z, ratio))
                ratio, up, down = call(
                    ratio_kernel,
                    ((2,) + block, edge_z, edge_z),
                    (taps_z, wide, fwd_x[n], fwd_y[n], back_y[n], *held[n]),
                    scratch=((planes, wide_rows, width_y), block),
                )
                ratios.append((move(up, z_up), ratio, move(down, z_down)))
            mids, lows, highs = [], [], []
            for s in range(outer):
                smeared, up, down = call(
                    back_z_kernel, ((2,) + block, edge_x, edge_x), (kern[2 * s : 2 * s + 2, 0], *ratios[s])
                )
                mids.append(smeared)
                lows.append(move(up, x_up))
                highs.append(move(down, x_down))
            estimate, up, down = call(
                update_kernel,
                (block, (planes, radius, width_y), (planes, radius, width_y)),
                (odd, back_x, estimate, *mids, *lows, *highs),
            )

        half = planes // 2
        result = jnp.zeros((planes, width_x, width_y), jnp.float32)
        across = [((A, C, K, B), (A, 1 - C, K, B)) for A, C, K, B in devices]
        for s, t in slots:
            pairs = [((A, C, K, B), ((A + s) % outer, B ^ t, K, C)) for A, C, K, B in devices]
            piece = move(lax.dynamic_slice_in_dim(estimate, (b ^ t) * half, half, 0), pairs)
            twin = move(piece, across)
            from_a = (a - s) % outer
            result = lax.dynamic_update_slice(result, piece, (c * half, part_of(from_a, c ^ t) * rows, 0))
            result = lax.dynamic_update_slice(
                result, twin, ((1 - c) * half, part_of(from_a, (1 - c) ^ t) * rows, 0)
            )
        return result

    return on_device


def solution(mesh):
    return jax.shard_map(
        make_on_device(mesh),
        mesh=mesh,
        in_specs=(P("view", "gz", None, None), P("gz", None, None), P(), P("view")),
        out_specs=P("gz", None, None),
        check_vma=False,
    )
```
